256 devices in a mesh: gx: 8 (over z_lo, core), gy: 32 (over y, x, z_hi).
Axes of the slice: x: 4, y: 4, z: 8 (z_hi: 2, z_lo: 4; z = z_hi * 4 + z_lo), core: 2. Of those that a mesh axis runs over, the one named last changes fastest.
Arguments:
- data: float32 [128, 512, 128], P('gx', 'gy'), may hold values from -6 to 6
- precond: float32 [128, 512, 128], P('gx', 'gy'), may hold values from 0.5 to 2
- psf: float32 [8, 32, 17, 17, 17], P('gx', 'gy'), may hold values from -0.05 to 0.05
Outputs:
- model: float32 [128, 512, 128], P('gx', 'gy')
- residual: float32 [128, 512, 128], P('gx', 'gy')
The draws below stay inside these ranges and needn't reach their ends.
All inputs are finite; a program needn't handle non-finite values.
Results may differ from the reference program's by a relative error of at most 0.0003.
Values sent between devices are 32-bit elements; how exact they have to be, the bound alone decides.
No kernel may reach another device: no remote copies, remote signals or barrier semaphores. Data moves between devices by JAX's collectives and lax.ppermute only.
A program may use at most 64 MiB of HBM per device.

```python
import math
import jax
import jax.numpy as jnp
from jax import lax

CX = 16
CY = 16
NZ = 128
PSF = 17
ITERS = 2
NX = 128
NY = 512
N_GX = 8
N_GY = 32


def block_levels(own_key, dims, pieces, smallest, largest):
    def one(position, shards_of):
        steps = jax.random.uniform(jax.random.fold_in(jax.random.fold_in(own_key, 6), position), (shards_of,), jnp.float32, smallest / len(pieces), largest / len(pieces))
        return jnp.repeat(jnp.exp(steps), dims[position] // shards_of).reshape((-1,) + (1,) * (len(dims) - position - 1))

    loudness = one(*pieces[0])
    for cut in pieces[1:]:
        loudness = loudness * one(*cut)
    return loudness


def centred(stream_key, extent, spread, limit, cuts=(), kind=jnp.bfloat16):
    result = spread * jax.random.normal(stream_key, extent, jnp.float32)
    if cuts:
        result = result * block_levels(stream_key, extent, cuts, -0.22, 0.18)
    return jnp.clip(result, -limit, limit).astype(kind)


def setup_inputs(seed: int = 0) -> dict:
    keys = jax.random.split(jax.random.key(seed), 4)
    return {
        "data": centred(keys[0], (NX, NY, NZ), 1.0, 6.0, ((0, 8), (1, 32)), jnp.float32),
        "precond": jnp.clip(jnp.exp(math.log(2.0) - 1.3862944 * jax.random.uniform(keys[1], (NX, NY, NZ), jnp.float32) ** block_levels(keys[1], (NX, NY, NZ), ((0, 8), (1, 32)), -0.2, 0.2)), 0.5, 2.0),
        "psf": centred(keys[2], (N_GX, N_GY, PSF, PSF, PSF), 0.008, 0.05, ((0, 8), (1, 32)), jnp.float32),
    }


relaxation = 0.7


def node_spectrum(kernel, length_x, length_y, length_z, half):
    width = kernel.shape[0]
    flipped = kernel[::-1, ::-1, ::-1]
    placed = jnp.zeros((length_x, length_y, length_z), kernel.dtype).at[:width, :width, :width].set(flipped)
    return jnp.fft.fftn(jnp.roll(placed, (-half, -half, -half), axis=(0, 1, 2)))


def apply_operator(field, psf):
    width = psf.shape[2]
    half = width // 2
    padded = jnp.pad(field, half)
    length_x = CX + 2 * half
    length_y = CY + 2 * half
    length_z = NZ + 2 * half
    along_x = (jnp.arange(CX, dtype=jnp.float32) + 0.5) / CX
    along_y = (jnp.arange(CY, dtype=jnp.float32) + 0.5) / CY

    def one_tile(index):
        row = (index // N_GY).astype(jnp.int32)
        column = (index % N_GY).astype(jnp.int32)
        row_next = jnp.minimum(row + 1, N_GX - 1).astype(jnp.int32)
        column_next = jnp.minimum(column + 1, N_GY - 1).astype(jnp.int32)
        start = (row * CX).astype(jnp.int32)
        begin = (column * CY).astype(jnp.int32)
        region = lax.dynamic_slice(padded, (start, begin, jnp.int32(0)), (length_x, length_y, length_z))
        region_spectrum = jnp.fft.fftn(region)
        nodes = ((row, column, (1.0 - along_x)[:, None] * (1.0 - along_y)[None, :]),
                 (row_next, column, along_x[:, None] * (1.0 - along_y)[None, :]),
                 (row, column_next, (1.0 - along_x)[:, None] * along_y[None, :]),
                 (row_next, column_next, along_x[:, None] * along_y[None, :]))
        total = jnp.zeros((CX, CY, NZ), field.dtype)
        for node_row, node_column, weight in nodes:
            kernel = psf[node_row, node_column]
            spectrum = node_spectrum(kernel, length_x, length_y, length_z, half)
            full = jnp.real(jnp.fft.ifftn(region_spectrum * spectrum))
            inner = full[half:half + CX, half:half + CY, half:half + NZ]
            total = total + weight[:, :, None].astype(field.dtype) * inner.astype(field.dtype)
        return total

    tiles = lax.map(one_tile, jnp.arange(N_GX * N_GY, dtype=jnp.int32))
    tiles = tiles.reshape(N_GX, N_GY, CX, CY, NZ).transpose(0, 2, 1, 3, 4).reshape(NX, NY, NZ)
    return field + tiles


def reference(data, precond, psf):
    model = precond * data
    residual = data
    for sweep_index in range(ITERS):
        residual = data - apply_operator(model, psf)
        model = model + relaxation * precond * residual
    return model, residual
```

```python
import jax
import jax.numpy as jnp
from jax import lax
from jax.experimental import pallas as pl
from jax.experimental.pallas import tpu as pltpu
from jax.sharding import PartitionSpec as P

ITERS = 2
relaxation = 0.7

H = 8
TAPS = 17
T = 16
Z = 128
GROUP = 32
SPAN = 640
ROWS = 2 * TAPS * 8 * T
PACKED = 88
VMEM = pl.BlockSpec(memory_space=pltpu.VMEM)


def call(kernel, outs, scratch=(), limit=None):
    return pl.pallas_call(
        kernel,
        out_shape=outs,
        scratch_shapes=list(scratch),
        compiler_params=pltpu.CompilerParams(vmem_limit_bytes=limit),
    )


def f32(*shape):
    return jax.ShapeDtypeStruct(shape, jnp.float32)


def prepare(d_ref, p_ref, psf_ref, v_ref, up_ref, down_ref, t_ref):
    v = d_ref[...] * p_ref[...]
    v_ref[...] = v
    up_ref[...] = v[:, H:, :]
    down_ref[: T * H, :] = v[:, :H, :].reshape(T * H, Z)
    t_ref[...] = jnp.zeros_like(t_ref)
    for a in range(TAPS):
        t_ref[GROUP * a : GROUP * a + TAPS, :TAPS] = psf_ref[0, 0, a]
    turned = t_ref[...].T
    for u in range(5):
        down_ref[T * H + u * TAPS : T * H + (u + 1) * TAPS, :] = turned[:TAPS, u * 128 : (u + 1) * 128]
    down_ref[T * H + 5 * TAPS :, :] = jnp.zeros((PACKED - 5 * TAPS, Z), jnp.float32)


def pack_first(v_ref, before_ref, down_ref, after_ref, wide_ref, up_ref, low_ref):
    wide_ref[:, :H, :] = before_ref[...]
    wide_ref[:, H : H + T, :] = v_ref[...]
    wide_ref[:, H + T :, :] = after_ref[: T * H, :].reshape(T, H, Z)
    up_ref[...] = wide_ref[H:]
    low_ref[: H * GROUP, :] = wide_ref[:H].reshape(H * GROUP, Z)
    low_ref[H * GROUP : H * GROUP + PACKED, :] = down_ref[T * H :, :]
    low_ref[H * GROUP + PACKED :, :] = after_ref[T * H :, :]


def pack_next(v_ref, before_ref, after_ref, wide_ref, up_ref, low_ref):
    wide_ref[:, :H, :] = before_ref[...]
    wide_ref[:, H : H + T, :] = v_ref[...]
    wide_ref[:, H + T :, :] = after_ref[...]
    up_ref[...] = wide_ref[H:]
    low_ref[...] = wide_ref[:H]


def halves(v):
    high = v.astype(jnp.bfloat16)
    low = (v - high.astype(jnp.float32)).astype(jnp.bfloat16)
    return jnp.concatenate([high, low], axis=1)


def stationary(v):
    both = halves(v)
    return jnp.concatenate([both, both], axis=0)


def slot(term, m, r, u):
    return ((term * 2 + m) * 4 + r) * 5 + u


def build(own_ref, nextx_ref, nexty_ref, corner_ref, wa_ref, wb_ref, rows_ref, last_x, last_y):
    def spread(ref):
        full = [ref[u * TAPS : (u + 1) * TAPS, :] for u in range(5)]
        return jnp.concatenate(full, axis=1)

    own = spread(own_ref)
    nextx = jnp.where(last_x, own, spread(nextx_ref))
    nexty = jnp.where(last_y, own, spread(nexty_ref))
    corner = jnp.where(last_y, nextx, jnp.where(last_x, nexty, spread(corner_ref)))
    for m, (near, far) in enumerate(((own, nexty), (nextx, corner))):
        for term, table in enumerate((near, far - near)):
            for r in range(4):
                rolled = table if r == 0 else pltpu.roll(table, GROUP * r, 1)
                for u in range(5):
                    rows_ref[slot(term, m, r, u), :TAPS, :] = rolled[:, u * 128 : (u + 1) * 128]
    along = lax.broadcasted_iota(jnp.int32, (H, Z), 0).astype(jnp.float32)
    steps = [(along + (0.5 + H * half)) / T for half in range(2)]
    zero = jnp.zeros((T, 128), jnp.bfloat16)

    @pl.loop(0, TAPS)
    def _(c):
        def base(x):
            return pl.multiple_of((((x // 8) * TAPS + c) * 8 + x % 8) * T, T)

        for r in range(4):
            for u in range(5):
                node = []
                for m in range(2):
                    near = rows_ref[slot(0, m, r, u), pl.ds(c, H, stride=0), :]
                    step = rows_ref[slot(1, m, r, u), pl.ds(c, H, stride=0), :]
                    node.append(
                        jnp.concatenate(
                            [
                                pltpu.roll(near + steps[half] * step, H * half, 1, stride=1, stride_axis=0)
                                for half in range(2)
                            ],
                            axis=0,
                        )
                    )
                across = node[1] - node[0]
                for q in range(4):
                    x = 4 * q + r
                    w = node[0] + ((x + 0.5) / T) * across
                    high = w.astype(jnp.bfloat16)
                    low = (w - high.astype(jnp.float32)).astype(jnp.bfloat16)
                    tile = q + u
                    if 2 <= tile < 6:
                        wa_ref[pl.ds(base(x), T), (tile - 2) * 128 : (tile - 1) * 128] = high
                        wa_ref[pl.ds(base(x), T), 512 + (tile - 2) * 128 : 512 + (tile - 1) * 128] = low
                    else:
                        at = (tile % 2) * 128
                        wb_ref[pl.ds(base(x), T), at : at + 128] = high
                        wb_ref[pl.ds(base(x), T), 256 + at : 256 + at + 128] = low
            for q, ref, at, width in ((0, wa_ref, 384, 512), (1, wb_ref, 0, 256), (2, wb_ref, 128, 256), (3, wa_ref, 0, 512)):
                ref[pl.ds(base(4 * q + r), T), at : at + 128] = zero
                ref[pl.ds(base(4 * q + r), T), width + at : width + at + 128] = zero


def product(w, v):
    both = jnp.dot(w, v, preferred_element_type=jnp.float32)
    return both[:, :Z] + both[:, Z:]


def inner_part(wide_ref, wa_ref, r_ref):
    v = stationary(wide_ref[...].reshape(T * GROUP, Z))
    for h in range(2):
        rows = slice(h * TAPS * 128, (h + 1) * TAPS * 128)
        r_ref[rows, :] = product(wa_ref[rows, :], v)


def outer_part(before_ref, after_ref, wb_ref, r_ref, out_ref):
    lane = lax.broadcasted_iota(jnp.int32, (128, Z), 1)
    for h, side in enumerate((before_ref, after_ref)):
        v = stationary(side[...])
        total = None
        for c in range(TAPS):
            at = slice((h * TAPS + c) * 128, (h * TAPS + c + 1) * 128)
            part = r_ref[at, :] + product(wb_ref[at, :], v)
            if c != H:
                part = pltpu.roll(part, (H - c) % Z, 1)
                part = jnp.where((lane >= H - c) & (lane < Z + H - c), part, 0.0)
            total = part if total is None else total + part
        out_ref[h * 8 : (h + 1) * 8] = total.reshape(8, T, Z)


def step_one(d_ref, p_ref, wide_ref, before_ref, low_ref, down_ref, nexty_ref, flag_ref,
             wa_ref, wb_ref, model_ref, rows_ref, r_ref, k_ref):
    last_x = flag_ref[0] == 1
    last_y = flag_ref[1] == 1
    side = H * GROUP
    build(
        down_ref.at[T * H :, :],
        low_ref.at[side : side + PACKED, :],
        nexty_ref.at[T * H :, :],
        low_ref.at[side + PACKED :, :],
        wa_ref, wb_ref, rows_ref, last_x, last_y,
    )
    inner_part(wide_ref, wa_ref, r_ref)
    outer_part(before_ref, low_ref.at[:side, :], wb_ref, r_ref, k_ref)
    v = wide_ref[:, H : H + T, :]
    residual = d_ref[...] - (v + k_ref[...])
    model_ref[...] = v + relaxation * p_ref[...] * residual


def step_two_inner(wide_ref, wa_ref, r_ref):
    inner_part(wide_ref, wa_ref, r_ref)


def step_two_outer(d_ref, p_ref, v_ref, before_ref, after_ref, wb_ref, r_ref, model_ref, residual_ref, k_ref):
    outer_part(before_ref, after_ref, wb_ref, r_ref, k_ref)
    v = v_ref[...]
    residual = d_ref[...] - (v + k_ref[...])
    residual_ref[...] = residual
    model_ref[...] = v + relaxation * p_ref[...] * residual


def passed_along(shard, axis, by):
    length = lax.axis_size(axis)
    return lax.ppermute(shard, axis, [(i, i + by) for i in range(length) if 0 <= i + by < length])


def pinned(shape, dtype):
    return pltpu.VMEM(shape, dtype)


def local(data, precond, psf):
    flags = jnp.stack([lax.axis_index("gx") == lax.axis_size("gx") - 1, lax.axis_index("gy") == lax.axis_size("gy") - 1]).astype(jnp.int32)
    v, up, down = call(
        prepare, (f32(T, T, Z), f32(T, H, Z), f32(T * H + PACKED, Z)), [pltpu.VMEM((SPAN, 128), jnp.float32)]
    )(data, precond, psf)
    before = passed_along(up, "gy", 1)
    after = passed_along(down, "gy", -1)
    wide, up, low = call(pack_first, (f32(T, GROUP, Z), f32(H, GROUP, Z), f32(H * GROUP + 2 * PACKED, Z)))(v, before, down, after)
    above = passed_along(up, "gx", 1)
    below = passed_along(low, "gx", -1)
    smem = pl.BlockSpec(memory_space=pltpu.SMEM)
    wa, wb, v = pl.pallas_call(
        step_one,
        out_shape=(
            pinned((ROWS, 1024), jnp.bfloat16),
            pinned((ROWS, 512), jnp.bfloat16),
            f32(T, T, Z),
        ),
        in_specs=[VMEM] * 7 + [smem],
        out_specs=(VMEM, VMEM, VMEM),
        scratch_shapes=[
            pltpu.VMEM((80, 24, 128), jnp.float32),
            pltpu.VMEM((ROWS, Z), jnp.float32),
            pltpu.VMEM((T, T, Z), jnp.float32),
        ],
        compiler_params=pltpu.CompilerParams(vmem_limit_bytes=40 << 20),
    )(data, precond, wide, above.reshape(H * GROUP, Z), below, down, after, flags)
    before = passed_along(v[:, H:, :], "gy", 1)
    after = passed_along(v[:, :H, :], "gy", -1)
    wide, up, low = call(pack_next, (f32(T, GROUP, Z), f32(H, GROUP, Z), f32(H, GROUP, Z)))(v, before, after)
    above = passed_along(up, "gx", 1)
    below = passed_along(low, "gx", -1)
    part = pl.pallas_call(
        step_two_inner,
        out_shape=pinned((ROWS, Z), jnp.float32),
        in_specs=[VMEM, VMEM],
        out_specs=VMEM,
        compiler_params=pltpu.CompilerParams(vmem_limit_bytes=24 << 20),
    )(wide, wa)
    return pl.pallas_call(
        step_two_outer,
        out_shape=(f32(T, T, Z), f32(T, T, Z)),
        in_specs=[VMEM] * 7,
        out_specs=(VMEM, VMEM),
        scratch_shapes=[pltpu.VMEM((T, T, Z), jnp.float32)],
        compiler_params=pltpu.CompilerParams(vmem_limit_bytes=16 << 20),
    )(data, precond, v, above.reshape(H * GROUP, Z), below.reshape(H * GROUP, Z), wb, part)


def solution(mesh):
    placed = (P("gx", "gy", None), P("gx", "gy", None), P("gx", "gy", None, None, None))
    return jax.shard_map(
        local,
        mesh=mesh,
        in_specs=placed,
        out_specs=(P("gx", "gy", None), P("gx", "gy", None)),
        check_vma=False,
    )
```

```python
import jax
import jax.numpy as jnp
from jax import lax
from jax.experimental import pallas as pl
from jax.experimental.pallas import tpu as pltpu
from jax.sharding import PartitionSpec as P

ITERS = 2
relaxation = 0.7

H = 8
TAPS = 17
T = 16
Z = 128
GROUP = 32
SPAN = 640
ROWS = 2 * TAPS * 8 * T
PACKED = 88
VMEM = pl.BlockSpec(memory_space=pltpu.VMEM)
MIB = 1 << 20


def held(*shape, dtype=jnp.float32):
    return pltpu.VMEM(shape, dtype)


def keep(x):
    return pltpu.with_memory_space_constraint(x, pltpu.VMEM)


def call(kernel, outs, mib, scratch=()):
    def run(*operands):
        return pl.pallas_call(
            kernel,
            out_shape=outs,
            in_specs=[VMEM] * len(operands),
            out_specs=jax.tree.map(lambda _: VMEM, outs),
            scratch_shapes=list(scratch),
            compiler_params=pltpu.CompilerParams(vmem_limit_bytes=int(mib * MIB)),
        )(*operands)

    return run


def even(axis):
    return lax.axis_index(axis) % 2 == 0


def last(axis):
    return lax.axis_index(axis) == lax.axis_size(axis) - 1


def swapped(axis, first, second):
    size = lax.axis_size(axis)
    received = []
    for start, sent in ((0, first), (1, second)):
        pairs = []
        for i in range(start, size - 1, 2):
            pairs += [(i, i + 1), (i + 1, i)]
        received.append(lax.ppermute(sent, axis, pairs))
    return received


def by_parity(axis, action):
    pl.when(even(axis))(lambda: action(0, 1))
    pl.when(jnp.logical_not(even(axis)))(lambda: action(1, 0))


def f32(*shape):
    return jax.ShapeDtypeStruct(shape, jnp.float32)


def prepare(d_ref, p_ref, psf_ref, v_ref, first_ref, second_ref, d_out_ref, p_out_ref, t_ref):
    d_out_ref[...] = d_ref[...]
    p_out_ref[...] = p_ref[...]
    v = d_ref[...] * p_ref[...]
    v_ref[...] = v
    t_ref[...] = jnp.zeros_like(t_ref)
    for a in range(TAPS):
        t_ref[GROUP * a : GROUP * a + TAPS, :TAPS] = psf_ref[0, 0, a]
    turned = t_ref[...].T
    sent = (first_ref, second_ref)
    for ref in sent:
        for u in range(5):
            ref[T * H + u * TAPS : T * H + (u + 1) * TAPS, :] = turned[:TAPS, u * 128 : (u + 1) * 128]
        ref[T * H + 5 * TAPS :, :] = jnp.zeros((PACKED - 5 * TAPS, Z), jnp.float32)

    def place(onward, back):
        sent[onward][: T * H, :] = v_ref[:, H:, :].reshape(T * H, Z)
        sent[back][: T * H, :] = v_ref[:, :H, :].reshape(T * H, Z)

    by_parity("gy", place)


def widen(v_ref, arrived, wide_ref):
    wide_ref[:, H : H + T, :] = v_ref[...]

    def place(onward, back):
        wide_ref[:, :H, :] = arrived[back][: T * H, :].reshape(T, H, Z)
        wide_ref[:, H + T :, :] = arrived[onward][: T * H, :].reshape(T, H, Z)

    by_parity("gy", place)


def pack_first(v_ref, own_ref, a_ref, b_ref, wide_ref, first_ref, second_ref):
    widen(v_ref, (a_ref, b_ref), wide_ref)
    sent = (first_ref, second_ref)
    side = H * GROUP

    def kernels(onward, back):
        for ref in sent:
            ref[side : side + PACKED, :] = own_ref[T * H :, :]
            ref[side + PACKED :, :] = jnp.where(last("gy"), own_ref[T * H :, :], (a_ref, b_ref)[onward][T * H :, :])

    by_parity("gy", kernels)

    def place(onward, back):
        sent[onward][:side, :] = wide_ref[H:].reshape(side, Z)
        sent[back][:side, :] = wide_ref[:H].reshape(side, Z)

    by_parity("gx", place)


def pack_next(v_ref, a_ref, b_ref, wide_ref, first_ref, second_ref):
    widen(v_ref, (a_ref, b_ref), wide_ref)
    sent = (first_ref, second_ref)
    side = H * GROUP

    def place(onward, back):
        sent[onward][...] = wide_ref[H:].reshape(side, Z)
        sent[back][...] = wide_ref[:H].reshape(side, Z)

    by_parity("gx", place)


def halves(v):
    high = v.astype(jnp.bfloat16)
    low = (v - high.astype(jnp.float32)).astype(jnp.bfloat16)
    return jnp.concatenate([high, low], axis=1)


def stationary(v):
    both = halves(v)
    return jnp.concatenate([both, both], axis=0)


def slot(term, m, r, u):
    return ((term * 2 + m) * 4 + r) * 5 + u


def spread(ref, at):
    return jnp.concatenate([ref[at + u * TAPS : at + (u + 1) * TAPS, :] for u in range(5)], axis=1)


def build(mine_ref, arrived, wa_ref, wb_ref, rows_ref):
    side = H * GROUP
    own, nexty = spread(mine_ref, side), spread(mine_ref, side + PACKED)
    onward = [jnp.where(even("gx"), spread(arrived[0], side + k * PACKED), spread(arrived[1], side + k * PACKED)) for k in range(2)]
    nextx, corner = jnp.where(last("gx"), own, onward[0]), jnp.where(last("gx"), nexty, onward[1])
    for m, (near, far) in enumerate(((own, nexty), (nextx, corner))):
        for term, table in enumerate((near, far - near)):
            for r in range(4):
                rolled = table if r == 0 else pltpu.roll(table, GROUP * r, 1)
                for u in range(5):
                    rows_ref[slot(term, m, r, u), :TAPS, :] = rolled[:, u * 128 : (u + 1) * 128]
    along = lax.broadcasted_iota(jnp.int32, (H, Z), 0).astype(jnp.float32)
    steps = [(along + (0.5 + H * half)) / T for half in range(2)]
    zero = jnp.zeros((T, 128), jnp.bfloat16)

    @pl.loop(0, TAPS)
    def _(c):
        def base(x):
            return pl.multiple_of((((x // 8) * TAPS + c) * 8 + x % 8) * T, T)

        for r in range(4):
            for u in range(5):
                node = []
                for m in range(2):
                    near = rows_ref[slot(0, m, r, u), pl.ds(c, H, stride=0), :]
                    step = rows_ref[slot(1, m, r, u), pl.ds(c, H, stride=0), :]
                    node.append(
                        jnp.concatenate(
                            [
                                pltpu.roll(near + steps[half] * step, H * half, 1, stride=1, stride_axis=0)
                                for half in range(2)
                            ],
                            axis=0,
                        )
                    )
                across = node[1] - node[0]
                for q in range(4):
                    x = 4 * q + r
                    w = node[0] + ((x + 0.5) / T) * across
                    high = w.astype(jnp.bfloat16)
                    low = (w - high.astype(jnp.float32)).astype(jnp.bfloat16)
                    tile = q + u
                    if 2 <= tile < 6:
                        wa_ref[pl.ds(base(x), T), (tile - 2) * 128 : (tile - 1) * 128] = high
                        wa_ref[pl.ds(base(x), T), 512 + (tile - 2) * 128 : 512 + (tile - 1) * 128] = low
                    else:
                        at = (tile % 2) * 128
                        wb_ref[pl.ds(base(x), T), at : at + 128] = high
                        wb_ref[pl.ds(base(x), T), 256 + at : 256 + at + 128] = low
            for q, ref, at, width in ((0, wa_ref, 384, 512), (1, wb_ref, 0, 256), (2, wb_ref, 128, 256), (3, wa_ref, 0, 512)):
                ref[pl.ds(base(4 * q + r), T), at : at + 128] = zero
                ref[pl.ds(base(4 * q + r), T), width + at : width + at + 128] = zero


def product(w, v):
    both = jnp.dot(w, v, preferred_element_type=jnp.float32)
    return both[:, :Z] + both[:, Z:]


def inner_part(wide_ref, wa_ref, r_ref):
    v = stationary(wide_ref[...].reshape(T * GROUP, Z))
    for h in range(2):
        rows = slice(h * TAPS * 128, (h + 1) * TAPS * 128)
        r_ref[rows, :] = product(wa_ref[rows, :], v)


def outer_part(arrived, wb_ref, r_ref, out_ref, side_ref):
    lane = lax.broadcasted_iota(jnp.int32, (128, Z), 1)

    def place(onward, back):
        side_ref[0] = arrived[back][: H * GROUP, :]
        side_ref[1] = arrived[onward][: H * GROUP, :]

    by_parity("gx", place)
    for h in range(2):
        v = stationary(side_ref[h])
        total = None
        for c in range(TAPS):
            at = slice((h * TAPS + c) * 128, (h * TAPS + c + 1) * 128)
            part = r_ref[at, :] + product(wb_ref[at, :], v)
            if c != H:
                part = pltpu.roll(part, (H - c) % Z, 1)
                part = jnp.where((lane >= H - c) & (lane < Z + H - c), part, 0.0)
            total = part if total is None else total + part
        out_ref[h * 8 : (h + 1) * 8] = total.reshape(8, T, Z)


def step_one(d_ref, p_ref, wide_ref, mine_ref, a_ref, b_ref,
             wa_ref, wb_ref, model_ref, first_ref, second_ref, rows_ref, r_ref, k_ref, side_ref):
    build(mine_ref, (a_ref, b_ref), wa_ref, wb_ref, rows_ref)
    inner_part(wide_ref, wa_ref, r_ref)
    outer_part((a_ref, b_ref), wb_ref, r_ref, k_ref, side_ref)
    v = wide_ref[:, H : H + T, :]
    residual = d_ref[...] - (v + k_ref[...])
    model_ref[...] = v + relaxation * p_ref[...] * residual
    sent = (first_ref, second_ref)

    def place(onward, back):
        sent[onward][...] = model_ref[:, H:, :].reshape(T * H, Z)
        sent[back][...] = model_ref[:, :H, :].reshape(T * H, Z)

    by_parity("gy", place)


def step_two(d_ref, p_ref, v_ref, a_ref, b_ref, wb_ref, r_ref, model_ref, residual_ref, k_ref, side_ref):
    outer_part((a_ref, b_ref), wb_ref, r_ref, k_ref, side_ref)
    v = v_ref[...]
    residual = d_ref[...] - (v + k_ref[...])
    residual_ref[...] = residual
    model_ref[...] = v + relaxation * p_ref[...] * residual


def local(data, precond, psf):
    side = H * GROUP
    wide_shape = held(T, GROUP, Z)
    block = pltpu.VMEM((T, T, Z), jnp.float32)
    sides = pltpu.VMEM((2, side, Z), jnp.float32)
    row = held(T * H + PACKED, Z)
    tile = held(T, T, Z)
    v, first, second, data, precond = call(prepare, (tile, row, row, tile, tile), 4, [pltpu.VMEM((SPAN, 128), jnp.float32)])(
        data, precond, psf
    )
    a, b = swapped("gy", first, second)
    row = held(side + 2 * PACKED, Z)
    wide, first, second = call(pack_first, (wide_shape, row, row), 3)(*map(keep, (v, first, a, b)))
    a, b = swapped("gx", first, second)
    row = held(T * H, Z)
    wa, wb, v, first, second = call(
        step_one,
        (held(ROWS, 1024, dtype=jnp.bfloat16), held(ROWS, 512, dtype=jnp.bfloat16), held(T, T, Z), row, row),
        14,
        [pltpu.VMEM((80, 24, 128), jnp.float32), pltpu.VMEM((ROWS, Z), jnp.float32), block, sides],
    )(*map(keep, (data, precond, wide, first, a, b)))
    a, b = swapped("gy", first, second)
    row = held(side, Z)
    wide, first, second = call(pack_next, (wide_shape, row, row), 3)(*map(keep, (v, a, b)))
    a, b = swapped("gx", first, second)
    part = call(inner_part, held(ROWS, Z), 8)(*map(keep, (wide, wa)))
    return call(step_two, (f32(T, T, Z), f32(T, T, Z)), 6, [block, sides])(
        *map(keep, (data, precond, v, a, b, wb, part))
    )


def solution(mesh):
    placed = (P("gx", "gy", None), P("gx", "gy", None), P("gx", "gy", None, None, None))
    return jax.shard_map(
        local,
        mesh=mesh,
        in_specs=placed,
        out_specs=(P("gx", "gy", None), P("gx", "gy", None)),
        check_vma=False,
    )
```

```python
import jax
import jax.numpy as jnp
from jax import lax
from jax.experimental import pallas as pl
from jax.experimental.pallas import tpu as pltpu
from jax.sharding import PartitionSpec as P


relaxation = 0.7

H = 8
TAPS = 17
T = 16
Z = 128
GROUP = 32
DENSE = TAPS * TAPS
ROWS = 2 * TAPS * 8 * T
PACKED = 40
FOLD = 40
VMEM = pl.BlockSpec(memory_space=pltpu.VMEM)
MIB = 1 << 20


def held(*shape, dtype=jnp.float32):
    return pltpu.VMEM(shape, dtype)


def keep(x):
    return pltpu.with_memory_space_constraint(x, pltpu.VMEM)


def call(kernel, outs, mib, scratch=(), space=VMEM):
    def run(*operands):
        return pl.pallas_call(
            kernel,
            out_shape=outs,
            in_specs=[space] * len(operands),
            out_specs=jax.tree.map(lambda _: VMEM, outs),
            scratch_shapes=list(scratch),
            compiler_params=pltpu.CompilerParams(vmem_limit_bytes=int(mib * MIB)),
        )(*operands)

    return run


def even(axis):
    return lax.axis_index(axis) % 2 == 0


def last(axis):
    return lax.axis_index(axis) == lax.axis_size(axis) - 1


def swapped(axis, first, second):
    size = lax.axis_size(axis)
    received = []
    for start, sent in ((0, first), (1, second)):
        pairs = []
        for i in range(start, size - 1, 2):
            pairs += [(i, i + 1), (i + 1, i)]
        received.append(lax.ppermute(sent, axis, pairs))
    return received


def by_parity(axis, action):
    pl.when(even(axis))(lambda: action(0, 1))
    pl.when(jnp.logical_not(even(axis)))(lambda: action(1, 0))


def f32(*shape):
    return jax.ShapeDtypeStruct(shape, jnp.float32)


def prepare(d_hbm, p_hbm, psf_hbm, v_ref, first_ref, second_ref, d_ref, p_ref, psf_ref, t_ref, sems):
    copies = [
        pltpu.make_async_copy(src, dst, sems.at[k])
        for k, (src, dst) in enumerate(((psf_hbm, psf_ref), (d_hbm, d_ref), (p_hbm, p_ref)))
    ]
    for copy in copies:
        copy.start()
    t_ref[DENSE:, :] = jnp.zeros((384 - DENSE, 128), jnp.float32)
    copies[0].wait()
    t_ref[:DENSE, :TAPS] = psf_ref[:, 0, :]
    turned = t_ref[...].T
    sent = (first_ref, second_ref)
    rest = turned[:TAPS, 256:]
    rest = jnp.where(lax.broadcasted_iota(jnp.int32, rest.shape, 1) < DENSE - 256, rest, 0.0)
    for ref in sent:
        at = T * H
        ref[at : at + TAPS, :] = turned[:TAPS, :128]
        ref[at + TAPS : at + 2 * TAPS, :] = turned[:TAPS, 128:256]
        ref[at + 34 : at + 40, :] = rest[:6] + pltpu.roll(rest, FOLD, 1)[6:12]
        ref[at + 34 : at + 39, :] += pltpu.roll(rest, 2 * FOLD, 1)[12:17]
    copies[1].wait()
    copies[2].wait()
    v_ref[...] = d_ref[...] * p_ref[...]

    def place(onward, back):
        sent[onward][: T * H, :] = v_ref[:, H:, :].reshape(T * H, Z)
        sent[back][: T * H, :] = v_ref[:, :H, :].reshape(T * H, Z)

    by_parity("gy", place)


def widen(v_ref, arrived, wide_ref):
    wide_ref[:, H : H + T, :] = v_ref[...]

    def place(onward, back):
        wide_ref[:, :H, :] = arrived[back][: T * H, :].reshape(T, H, Z)
        wide_ref[:, H + T :, :] = arrived[onward][: T * H, :].reshape(T, H, Z)

    by_parity("gy", place)


def pack_first(v_ref, own_ref, a_ref, b_ref, wide_ref, first_ref, second_ref):
    widen(v_ref, (a_ref, b_ref), wide_ref)
    sent = (first_ref, second_ref)
    side = H * GROUP

    def kernels(onward, back):
        for ref in sent:
            ref[side : side + PACKED, :] = own_ref[T * H :, :]
            ref[side + PACKED :, :] = jnp.where(last("gy"), own_ref[T * H :, :], (a_ref, b_ref)[onward][T * H :, :])

    by_parity("gy", kernels)

    def place(onward, back):
        sent[onward][:side, :] = wide_ref[H:].reshape(side, Z)
        sent[back][:side, :] = wide_ref[:H].reshape(side, Z)

    by_parity("gx", place)


def pack_next(v_ref, a_ref, b_ref, wide_ref, first_ref, second_ref):
    widen(v_ref, (a_ref, b_ref), wide_ref)
    sent = (first_ref, second_ref)
    side = H * GROUP

    def place(onward, back):
        sent[onward][...] = wide_ref[H:].reshape(side, Z)
        sent[back][...] = wide_ref[:H].reshape(side, Z)

    by_parity("gx", place)


def halves(v):
    high = v.astype(jnp.bfloat16)
    low = (v - high.astype(jnp.float32)).astype(jnp.bfloat16)
    return jnp.concatenate([high, low], axis=1)


def stationary(v):
    both = halves(v)
    return jnp.concatenate([both, both], axis=0)


def expanded(rows):
    fold = rows[34:40]
    source = (
        rows[:TAPS],
        rows[TAPS : 2 * TAPS],
        jnp.concatenate([fold, pltpu.roll(fold, 128 - FOLD, 1), pltpu.roll(fold, 128 - 2 * FOLD, 1)[:5]], axis=0),
    )
    lane = lax.broadcasted_iota(jnp.int32, (TAPS, 128), 1)
    tiles = []
    for u in range(5):
        tile = jnp.zeros((TAPS, 128), jnp.float32)
        for a in range(4 * u, min(4 * u + 4, TAPS)):
            begin, to = TAPS * a, GROUP * (a % 4)
            for k in sorted({begin // 128, (begin + TAPS - 1) // 128}):
                low, high = max(begin, 128 * k), min(begin + TAPS, 128 * (k + 1))
                shift = (to - begin) % 128
                moved = pltpu.roll(source[k], shift, 1) if shift else source[k]
                tile = jnp.where((lane >= to + low - begin) & (lane < to + high - begin), moved, tile)
        tiles.append(tile)
    return jnp.concatenate(tiles, axis=1)


def shifted(table, rows_ref, k):
    for r in range(4):
        rolled = table if r == 0 else pltpu.roll(table, GROUP * r, 1)
        for u in range(5):
            rows_ref[(k * 4 + r) * 5 + u, :TAPS, :] = rolled[:, u * 128 : (u + 1) * 128]


def own_rows(mine_ref, rows_ref):
    side = H * GROUP
    own, nexty = mine_ref[side : side + PACKED, :], mine_ref[side + PACKED :, :]
    for k, rows in enumerate((own, nexty - own)):
        shifted(expanded(rows), rows_ref, k)


def build(mine_ref, arrived, own_rows_ref, wa_ref, wb_ref, rows_ref, even_ref, odd_ref):
    side = H * GROUP
    own, nexty = mine_ref[side : side + PACKED, :], mine_ref[side + PACKED :, :]
    onward = jnp.where(even("gx"), arrived[0][side:, :], arrived[1][side:, :])
    nextx, corner = jnp.where(last("gx"), own, onward[:PACKED]), jnp.where(last("gx"), nexty, onward[PACKED:])
    across = nextx - own
    for k, rows in enumerate((across, corner - nexty - across)):
        shifted(expanded(0.25 * rows), rows_ref, 2 + k)
    for k in range(2):
        for r in range(4):
            for u in range(5):
                at = (k * 4 + r) * 5 + u
                rows_ref[at] = own_rows_ref[at] + ((r + 0.5) / 4) * rows_ref[at + 40]
    along = lax.broadcasted_iota(jnp.int32, (H, Z), 0).astype(jnp.float32)
    steps = [(along + (0.5 + H * half)) / T for half in range(2)]
    zero = jnp.zeros((T, 128), jnp.bfloat16)

    def spread(c, q_ref):
        for r in range(4):
            for u in range(5):
                for m in range(2):
                    at = (m * 8 + r) * 5 + u
                    near = rows_ref[at, pl.ds(c, H, stride=0), :]
                    step = rows_ref[at + 20, pl.ds(c, H, stride=0), :]
                    for half in range(2):
                        q_ref[m, r * 5 + u, half * H : (half + 1) * H, :] = pltpu.roll(
                            near + steps[half] * step, H * half, 1, stride=1, stride_axis=0
                        )

    def fill(c, q_ref):
        def base(x):
            return pl.multiple_of((((x // 8) * TAPS + c) * 8 + x % 8) * T, T)

        for r in range(4):
            for u in range(5):
                w, quarter = q_ref[0, r * 5 + u], q_ref[1, r * 5 + u]
                for q in range(4):
                    w = w if q == 0 else w + quarter
                    high = w.astype(jnp.bfloat16)
                    low = (w - high.astype(jnp.float32)).astype(jnp.bfloat16)
                    tile = q + u
                    rows = pl.ds(base(4 * q + r), T)
                    ref, at, width = (wa_ref, tile - 2, 4) if 2 <= tile < 6 else (wb_ref, tile % 2, 2)
                    ref[at, rows, :] = high
                    ref[at + width, rows, :] = low
            for q, ref, at, width in ((0, wa_ref, 3, 4), (1, wb_ref, 0, 2), (2, wb_ref, 1, 2), (3, wa_ref, 0, 4)):
                rows = pl.ds(base(4 * q + r), T)
                ref[at, rows, :] = zero
                ref[at + width, rows, :] = zero

    spread(0, even_ref)

    @pl.loop(0, TAPS // 2)
    def _(i):
        spread(2 * i + 1, odd_ref)
        fill(2 * i, even_ref)
        spread(2 * i + 2, even_ref)
        fill(2 * i + 1, odd_ref)

    fill(TAPS - 1, even_ref)


def joined(ref, rows):
    return jnp.concatenate([ref[t, rows, :] for t in range(ref.shape[0])], axis=1)


def product(w, v):
    both = jnp.dot(w, v, preferred_element_type=jnp.float32)
    return both[:, :Z] + both[:, Z:]


def inner_part(wide_ref, wa_ref, r_ref):
    v = stationary(wide_ref[...].reshape(T * GROUP, Z))
    for h in range(2):
        rows = slice(h * TAPS * 128, (h + 1) * TAPS * 128)
        r_ref[rows, :] = product(joined(wa_ref, rows), v)


def outer_part(arrived, wb_ref, r_ref, out_ref, side_ref):
    lane = lax.broadcasted_iota(jnp.int32, (128, Z), 1)

    def place(onward, back):
        side_ref[0] = arrived[back][: H * GROUP, :]
        side_ref[1] = arrived[onward][: H * GROUP, :]

    by_parity("gx", place)
    for h in range(2):
        v = stationary(side_ref[h])
        total = None
        for c in range(TAPS):
            at = slice((h * TAPS + c) * 128, (h * TAPS + c + 1) * 128)
            part = r_ref[at, :] + product(joined(wb_ref, at), v)
            if c != H:
                part = pltpu.roll(part, (H - c) % Z, 1)
                part = jnp.where((lane >= H - c) & (lane < Z + H - c), part, 0.0)
            total = part if total is None else total + part
        out_ref[h * 8 : (h + 1) * 8] = total.reshape(8, T, Z)


def step_one(d_ref, p_ref, wide_ref, mine_ref, a_ref, b_ref, own_rows_ref,
             wa_ref, wb_ref, model_ref, first_ref, second_ref, rows_ref, even_ref, odd_ref, r_ref, k_ref, side_ref):
    build(mine_ref, (a_ref, b_ref), own_rows_ref, wa_ref, wb_ref, rows_ref, even_ref, odd_ref)
    inner_part(wide_ref, wa_ref, r_ref)
    outer_part((a_ref, b_ref), wb_ref, r_ref, k_ref, side_ref)
    v = wide_ref[:, H : H + T, :]
    residual = d_ref[...] - (v + k_ref[...])
    model_ref[...] = v + relaxation * p_ref[...] * residual
    sent = (first_ref, second_ref)

    def place(onward, back):
        sent[onward][...] = model_ref[:, H:, :].reshape(T * H, Z)
        sent[back][...] = model_ref[:, :H, :].reshape(T * H, Z)

    by_parity("gy", place)


def step_two(d_ref, p_ref, v_ref, a_ref, b_ref, wb_ref, r_ref, model_ref, residual_ref, k_ref, side_ref):
    outer_part((a_ref, b_ref), wb_ref, r_ref, k_ref, side_ref)
    v = v_ref[...]
    residual = d_ref[...] - (v + k_ref[...])
    residual_ref[...] = residual
    model_ref[...] = v + relaxation * p_ref[...] * residual


def local(data, precond, psf):
    side = H * GROUP
    wide_shape = held(T, GROUP, Z)
    block = pltpu.VMEM((T, T, Z), jnp.float32)
    sides = pltpu.VMEM((2, side, Z), jnp.float32)
    row = held(T * H + PACKED, Z)
    tile = held(T, T, Z)
    psf = psf.reshape(DENSE, 1, TAPS)
    v, first, second, data, precond = call(
        prepare,
        (tile, row, row, tile, tile),
        4,
        [
            pltpu.VMEM((DENSE, 1, TAPS), jnp.float32),
            pltpu.VMEM((384, 128), jnp.float32),
            pltpu.SemaphoreType.DMA((3,)),
        ],
        pl.BlockSpec(memory_space=pltpu.HBM),
    )(*(pltpu.with_memory_space_constraint(x, pltpu.HBM) for x in (data, precond, psf)))
    a, b = swapped("gy", first, second)
    row = held(side + 2 * PACKED, Z)
    wide, first, second = call(pack_first, (wide_shape, row, row), 3)(*map(keep, (v, first, a, b)))
    a, b = swapped("gx", first, second)
    tables = call(own_rows, held(40, 24, 128), 2)(keep(first))
    row = held(T * H, Z)
    turned = pltpu.VMEM((2, 20, T, 128), jnp.float32)
    wa, wb, v, first, second = call(
        step_one,
        (held(8, ROWS, 128, dtype=jnp.bfloat16), held(4, ROWS, 128, dtype=jnp.bfloat16), held(T, T, Z), row, row),
        14,
        [pltpu.VMEM((80, 24, 128), jnp.float32), turned, turned, pltpu.VMEM((ROWS, Z), jnp.float32), block, sides],
    )(*map(keep, (data, precond, wide, first, a, b, tables)))
    a, b = swapped("gy", first, second)
    row = held(side, Z)
    wide, first, second = call(pack_next, (wide_shape, row, row), 3)(*map(keep, (v, a, b)))
    a, b = swapped("gx", first, second)
    part = call(inner_part, held(ROWS, Z), 8)(*map(keep, (wide, wa)))
    return call(step_two, (f32(T, T, Z), f32(T, T, Z)), 6, [block, sides])(
        *map(keep, (data, precond, v, a, b, wb, part))
    )


def solution(mesh):
    placed = (P("gx", "gy", None), P("gx", "gy", None), P("gx", "gy", None, None, None))
    return jax.shard_map(
        local,
        mesh=mesh,
        in_specs=placed,
        out_specs=(P("gx", "gy", None), P("gx", "gy", None)),
        check_vma=False,
    )
```

```python
import jax
import jax.numpy as jnp
from jax import lax
from jax.experimental import pallas as pl
from jax.experimental.pallas import tpu as pltpu
from jax.sharding import PartitionSpec as P


relaxation = 0.7

H = 8
TAPS = 17
T = 16
Z = 128
GROUP = 32
DENSE = TAPS * TAPS
ROWS = 2 * TAPS * 8 * T
PACKED = 40
FOLD = 40
VMEM = pl.BlockSpec(memory_space=pltpu.VMEM)
MIB = 1 << 20


def held(*shape, dtype=jnp.float32):
    return pltpu.VMEM(shape, dtype)


def keep(x):
    return pltpu.with_memory_space_constraint(x, pltpu.VMEM)


def call(kernel, outs, mib, scratch=(), space=VMEM):
    def run(*operands):
        return pl.pallas_call(
            kernel,
            out_shape=outs,
            in_specs=[space] * len(operands),
            out_specs=jax.tree.map(lambda _: VMEM, outs),
            scratch_shapes=list(scratch),
            compiler_params=pltpu.CompilerParams(vmem_limit_bytes=int(mib * MIB)),
        )(*operands)

    return run


def even(axis):
    return lax.axis_index(axis) % 2 == 0


def last(axis):
    return lax.axis_index(axis) == lax.axis_size(axis) - 1


def swapped(axis, first, second):
    size = lax.axis_size(axis)
    received = []
    for start, sent in ((0, first), (1, second)):
        pairs = []
        for i in range(start, size - 1, 2):
            pairs += [(i, i + 1), (i + 1, i)]
        received.append(lax.ppermute(sent, axis, pairs))
    return received


def by_parity(axis, action):
    pl.when(even(axis))(lambda: action(0, 1))
    pl.when(jnp.logical_not(even(axis)))(lambda: action(1, 0))


def f32(*shape):
    return jax.ShapeDtypeStruct(shape, jnp.float32)


def prepare(d_hbm, p_hbm, psf_hbm, v_ref, first_ref, second_ref, d_ref, p_ref, psf_ref, t_ref, sems):
    copies = [
        pltpu.make_async_copy(src, dst, sems.at[k])
        for k, (src, dst) in enumerate(((psf_hbm, psf_ref), (d_hbm, d_ref), (p_hbm, p_ref)))
    ]
    for copy in copies:
        copy.start()
    t_ref[DENSE:, :] = jnp.zeros((384 - DENSE, 128), jnp.float32)
    copies[0].wait()
    t_ref[:DENSE, :TAPS] = psf_ref[:, 0, :]
    turned = t_ref[...].T
    sent = (first_ref, second_ref)
    rest = turned[:TAPS, 256:]
    rest = jnp.where(lax.broadcasted_iota(jnp.int32, rest.shape, 1) < DENSE - 256, rest, 0.0)
    for ref in sent:
        at = T * H
        ref[at : at + TAPS, :] = turned[:TAPS, :128]
        ref[at + TAPS : at + 2 * TAPS, :] = turned[:TAPS, 128:256]
        ref[at + 34 : at + 40, :] = rest[:6] + pltpu.roll(rest, FOLD, 1)[6:12]
        ref[at + 34 : at + 39, :] += pltpu.roll(rest, 2 * FOLD, 1)[12:17]
    copies[1].wait()
    copies[2].wait()
    v_ref[...] = d_ref[...] * p_ref[...]

    def place(onward, back):
        sent[onward][: T * H, :] = v_ref[:, H:, :].reshape(T * H, Z)
        sent[back][: T * H, :] = v_ref[:, :H, :].reshape(T * H, Z)

    by_parity("gy", place)


def widen(v_ref, arrived, wide_ref):
    wide_ref[:, H : H + T, :] = v_ref[...]

    def place(onward, back):
        wide_ref[:, :H, :] = arrived[back][: T * H, :].reshape(T, H, Z)
        wide_ref[:, H + T :, :] = arrived[onward][: T * H, :].reshape(T, H, Z)

    by_parity("gy", place)


def pack_first(v_ref, own_ref, a_ref, b_ref, wide_ref, first_ref, second_ref):
    widen(v_ref, (a_ref, b_ref), wide_ref)
    sent = (first_ref, second_ref)
    side = H * GROUP

    def kernels(onward, back):
        for ref in sent:
            ref[side : side + PACKED, :] = own_ref[T * H :, :]
            ref[side + PACKED :, :] = jnp.where(last("gy"), own_ref[T * H :, :], (a_ref, b_ref)[onward][T * H :, :])

    by_parity("gy", kernels)

    def place(onward, back):
        sent[onward][:side, :] = wide_ref[H:].reshape(side, Z)
        sent[back][:side, :] = wide_ref[:H].reshape(side, Z)

    by_parity("gx", place)


def pack_next(v_ref, a_ref, b_ref, wide_ref, first_ref, second_ref):
    widen(v_ref, (a_ref, b_ref), wide_ref)
    sent = (first_ref, second_ref)
    side = H * GROUP

    def place(onward, back):
        sent[onward][...] = wide_ref[H:].reshape(side, Z)
        sent[back][...] = wide_ref[:H].reshape(side, Z)

    by_parity("gx", place)


def halves(v):
    high = v.astype(jnp.bfloat16)
    low = (v - high.astype(jnp.float32)).astype(jnp.bfloat16)
    return jnp.concatenate([high, low], axis=1)


def stationary(v):
    both = halves(v)
    return jnp.concatenate([both, both], axis=0)


def expanded(rows):
    fold = rows[34:40]
    source = (
        rows[:TAPS],
        rows[TAPS : 2 * TAPS],
        jnp.concatenate([fold, pltpu.roll(fold, 128 - FOLD, 1), pltpu.roll(fold, 128 - 2 * FOLD, 1)[:5]], axis=0),
    )
    lane = lax.broadcasted_iota(jnp.int32, (TAPS, 128), 1)
    tiles = []
    for u in range(5):
        tile = jnp.zeros((TAPS, 128), jnp.float32)
        for a in range(4 * u, min(4 * u + 4, TAPS)):
            begin, to = TAPS * a, GROUP * (a % 4)
            for k in sorted({begin // 128, (begin + TAPS - 1) // 128}):
                low, high = max(begin, 128 * k), min(begin + TAPS, 128 * (k + 1))
                shift = (to - begin) % 128
                moved = pltpu.roll(source[k], shift, 1) if shift else source[k]
                tile = jnp.where((lane >= to + low - begin) & (lane < to + high - begin), moved, tile)
        tiles.append(tile)
    return jnp.concatenate(tiles, axis=1)


def shifted(table, rows_ref, k):
    for r in range(4):
        rolled = table if r == 0 else pltpu.roll(table, GROUP * r, 1)
        for u in range(5):
            rows_ref[(k * 4 + r) * 5 + u, :TAPS, :] = rolled[:, u * 128 : (u + 1) * 128]


def own_rows(mine_ref, rows_ref):
    side = H * GROUP
    own, nexty = mine_ref[side : side + PACKED, :], mine_ref[side + PACKED :, :]
    for k, rows in enumerate((own, nexty - own)):
        shifted(expanded(rows), rows_ref, k)


def build(mine_ref, arrived, own_rows_ref, wa_ref, wb_ref, rows_ref, even_ref, odd_ref, use):
    side = H * GROUP
    own, nexty = mine_ref[side : side + PACKED, :], mine_ref[side + PACKED :, :]
    onward = jnp.where(even("gx"), arrived[0][side:, :], arrived[1][side:, :])
    nextx, corner = jnp.where(last("gx"), own, onward[:PACKED]), jnp.where(last("gx"), nexty, onward[PACKED:])
    across = nextx - own
    for k, rows in enumerate((across, corner - nexty - across)):
        shifted(expanded(0.25 * rows), rows_ref, 2 + k)
    for k in range(2):
        for r in range(4):
            for u in range(5):
                at = (k * 4 + r) * 5 + u
                rows_ref[at] = own_rows_ref[at] + ((r + 0.5) / 4) * rows_ref[at + 40]
    along = lax.broadcasted_iota(jnp.int32, (H, Z), 0).astype(jnp.float32)
    steps = [(along + (0.5 + H * half)) / T for half in range(2)]
    zero = jnp.zeros((T, 128), jnp.bfloat16)

    def spread(c, q_ref):
        for r in range(4):
            for u in range(5):
                for m in range(2):
                    at = (m * 8 + r) * 5 + u
                    near = rows_ref[at, pl.ds(c, H, stride=0), :]
                    step = rows_ref[at + 20, pl.ds(c, H, stride=0), :]
                    for half in range(2):
                        q_ref[m, r * 5 + u, half * H : (half + 1) * H, :] = pltpu.roll(
                            near + steps[half] * step, H * half, 1, stride=1, stride_axis=0
                        )

    def fill(c, q_ref):
        def base(x):
            return (((x // 8) * TAPS + c) * 8 + x % 8) * T

        for r in range(4):
            for u in range(5):
                w, quarter = q_ref[0, r * 5 + u], q_ref[1, r * 5 + u]
                for q in range(4):
                    w = w if q == 0 else w + quarter
                    high = w.astype(jnp.bfloat16)
                    low = (w - high.astype(jnp.float32)).astype(jnp.bfloat16)
                    tile = q + u
                    rows = pl.ds(base(4 * q + r), T)
                    ref, at, width = (wa_ref, tile - 2, 4) if 2 <= tile < 6 else (wb_ref, tile % 2, 2)
                    ref[at, rows, :] = high
                    ref[at + width, rows, :] = low
            for q, ref, at, width in ((0, wa_ref, 3, 4), (1, wb_ref, 0, 2), (2, wb_ref, 1, 2), (3, wa_ref, 0, 4)):
                rows = pl.ds(base(4 * q + r), T)
                ref[at, rows, :] = zero
                ref[at + width, rows, :] = zero

    held_refs = (even_ref, odd_ref)
    spread(0, even_ref)
    spread(1, odd_ref)
    fill(0, even_ref)
    for c in range(TAPS):
        use(c)
        if c + 1 < TAPS:
            fill(c + 1, held_refs[(c + 1) % 2])
        if c + 2 < TAPS:
            spread(c + 2, held_refs[c % 2])


def joined(ref, rows):
    return jnp.concatenate([ref[t, rows, :] for t in range(ref.shape[0])], axis=1)


def product(w, v):
    both = jnp.dot(w, v, preferred_element_type=jnp.float32)
    return both[:, :Z] + both[:, Z:]


def inner_part(wide_ref, wa_ref, r_ref):
    v = stationary(wide_ref[...].reshape(T * GROUP, Z))
    for h in range(2):
        rows = slice(h * TAPS * 128, (h + 1) * TAPS * 128)
        r_ref[rows, :] = product(joined(wa_ref, rows), v)


def moved(part, c):
    if c == H:
        return part
    lane = lax.broadcasted_iota(jnp.int32, part.shape, 1)
    return jnp.where((lane >= H - c) & (lane < Z + H - c), pltpu.roll(part, (H - c) % Z, 1), 0.0)


def sides(arrived, side_ref):
    def place(onward, back):
        side_ref[0] = arrived[back][: H * GROUP, :]
        side_ref[1] = arrived[onward][: H * GROUP, :]

    by_parity("gx", place)


def outer_part(arrived, wb_ref, r_ref, out_ref, side_ref):
    sides(arrived, side_ref)
    for h in range(2):
        v = stationary(side_ref[h])
        total = None
        for c in range(TAPS):
            at = slice((h * TAPS + c) * 128, (h * TAPS + c + 1) * 128)
            part = moved(r_ref[at, :] + product(joined(wb_ref, at), v), c)
            total = part if total is None else total + part
        out_ref[h * 8 : (h + 1) * 8] = total.reshape(8, T, Z)


def step_one(d_ref, p_ref, wide_ref, mine_ref, a_ref, b_ref, own_rows_ref,
             wa_ref, wb_ref, model_ref, first_ref, second_ref, rows_ref, even_ref, odd_ref, all_ref, k_ref, side_ref):
    sides((a_ref, b_ref), side_ref)
    inner = stationary(wide_ref[...].reshape(T * GROUP, Z))
    for h in range(2):
        all_ref[h, : 4 * 256, :] = inner
        all_ref[h, 4 * 256 :, :] = stationary(side_ref[h])

    def use(c):
        for h in range(2):
            at = slice((h * TAPS + c) * 128, (h * TAPS + c + 1) * 128)
            w = jnp.concatenate([joined(wa_ref, at), joined(wb_ref, at)], axis=1)
            part = moved(product(w, all_ref[h]), c)
            k_ref[h] = part if c == 0 else k_ref[h] + part

    build(mine_ref, (a_ref, b_ref), own_rows_ref, wa_ref, wb_ref, rows_ref, even_ref, odd_ref, use)
    v = wide_ref[:, H : H + T, :]
    residual = d_ref[...] - (v + k_ref[...].reshape(T, T, Z))
    model_ref[...] = v + relaxation * p_ref[...] * residual
    sent = (first_ref, second_ref)

    def place(onward, back):
        sent[onward][...] = model_ref[:, H:, :].reshape(T * H, Z)
        sent[back][...] = model_ref[:, :H, :].reshape(T * H, Z)

    by_parity("gy", place)


def step_two(d_ref, p_ref, v_ref, a_ref, b_ref, wb_ref, r_ref, model_ref, residual_ref, k_ref, side_ref):
    outer_part((a_ref, b_ref), wb_ref, r_ref, k_ref, side_ref)
    v = v_ref[...]
    residual = d_ref[...] - (v + k_ref[...])
    residual_ref[...] = residual
    model_ref[...] = v + relaxation * p_ref[...] * residual


def local(data, precond, psf):
    side = H * GROUP
    wide_shape = held(T, GROUP, Z)
    block = pltpu.VMEM((T, T, Z), jnp.float32)
    edges = pltpu.VMEM((2, side, Z), jnp.float32)
    row = held(T * H + PACKED, Z)
    tile = held(T, T, Z)
    psf = psf.reshape(DENSE, 1, TAPS)
    v, first, second, data, precond = call(
        prepare,
        (tile, row, row, tile, tile),
        4,
        [
            pltpu.VMEM((DENSE, 1, TAPS), jnp.float32),
            pltpu.VMEM((384, 128), jnp.float32),
            pltpu.SemaphoreType.DMA((3,)),
        ],
        pl.BlockSpec(memory_space=pltpu.HBM),
    )(*(pltpu.with_memory_space_constraint(x, pltpu.HBM) for x in (data, precond, psf)))
    a, b = swapped("gy", first, second)
    row = held(side + 2 * PACKED, Z)
    wide, first, second = call(pack_first, (wide_shape, row, row), 3)(*map(keep, (v, first, a, b)))
    a, b = swapped("gx", first, second)
    tables = call(own_rows, held(40, 24, 128), 2)(keep(first))
    row = held(T * H, Z)
    turned = pltpu.VMEM((2, 20, T, 128), jnp.float32)
    wa, wb, v, first, second = call(
        step_one,
        (held(8, ROWS, 128, dtype=jnp.bfloat16), held(4, ROWS, 128, dtype=jnp.bfloat16), held(T, T, Z), row, row),
        14,
        [
            pltpu.VMEM((80, 24, 128), jnp.float32),
            turned,
            turned,
            pltpu.VMEM((2, 6 * 256, 2 * Z), jnp.bfloat16),
            pltpu.VMEM((2, 128, Z), jnp.float32),
            edges,
        ],
    )(*map(keep, (data, precond, wide, first, a, b, tables)))
    a, b = swapped("gy", first, second)
    row = held(side, Z)
    wide, first, second = call(pack_next, (wide_shape, row, row), 3)(*map(keep, (v, a, b)))
    a, b = swapped("gx", first, second)
    part = call(inner_part, held(ROWS, Z), 8)(*map(keep, (wide, wa)))
    return call(step_two, (f32(T, T, Z), f32(T, T, Z)), 6, [block, edges])(
        *map(keep, (data, precond, v, a, b, wb, part))
    )


def solution(mesh):
    placed = (P("gx", "gy", None), P("gx", "gy", None), P("gx", "gy", None, None, None))
    return jax.shard_map(
        local,
        mesh=mesh,
        in_specs=placed,
        out_specs=(P("gx", "gy", None), P("gx", "gy", None)),
        check_vma=False,
    )
```

```python
import jax
import jax.numpy as jnp
from jax import lax
from jax.experimental import pallas as pl
from jax.experimental.pallas import tpu as pltpu
from jax.sharding import PartitionSpec as P


relaxation = 0.7

H = 8
TAPS = 17
T = 16
Z = 128
GROUP = 32
DENSE = TAPS * TAPS
ROWS = 2 * TAPS * 8 * T
PACKED = 40
FOLD = 40
VMEM = pl.BlockSpec(memory_space=pltpu.VMEM)
MIB = 1 << 20


def held(*shape, dtype=jnp.float32):
    return pltpu.VMEM(shape, dtype)


def keep(x):
    return pltpu.with_memory_space_constraint(x, pltpu.VMEM)


def call(kernel, outs, mib, scratch=(), space=VMEM, alias={}):
    def run(*operands):
        return pl.pallas_call(
            kernel,
            out_shape=outs,
            in_specs=[space] * len(operands),
            out_specs=jax.tree.map(lambda _: VMEM, outs),
            scratch_shapes=list(scratch),
            input_output_aliases=alias,
            compiler_params=pltpu.CompilerParams(vmem_limit_bytes=int(mib * MIB)),
        )(*operands)

    return run


def even(axis):
    return lax.axis_index(axis) % 2 == 0


def last(axis):
    return lax.axis_index(axis) == lax.axis_size(axis) - 1


def swapped(axis, first, second):
    size = lax.axis_size(axis)
    received = []
    for start, sent in ((0, first), (1, second)):
        pairs = []
        for i in range(start, size - 1, 2):
            pairs += [(i, i + 1), (i + 1, i)]
        received.append(lax.ppermute(sent, axis, pairs))
    return received


def by_parity(axis, action):
    pl.when(even(axis))(lambda: action(0, 1))
    pl.when(jnp.logical_not(even(axis)))(lambda: action(1, 0))


def f32(*shape):
    return jax.ShapeDtypeStruct(shape, jnp.float32)


def columns(v_ref, sent):
    def place(onward, back):
        sent[onward][: T * H, :] = v_ref[:, H:, :].reshape(T * H, Z)
        sent[back][: T * H, :] = v_ref[:, :H, :].reshape(T * H, Z)

    by_parity("gy", place)


def rows(v_ref, sent):
    def place(onward, back):
        sent[onward][: T * H, :] = v_ref[H:].reshape(T * H, Z)
        sent[back][: T * H, :] = v_ref[:H].reshape(T * H, Z)

    by_parity("gx", place)


def corners(wide_ref, sent):
    def place(onward, back):
        for ref, half in ((sent[onward], wide_ref.at[H:]), (sent[back], wide_ref.at[:H])):
            ref[: T * H, :] = jnp.concatenate([half[:, :H, :], half[:, H + T :, :]], axis=1).reshape(T * H, Z)

    by_parity("gx", place)


def prepare(d_hbm, p_hbm, psf_hbm, v_ref, first_ref, second_ref, xfirst_ref, xsecond_ref, d_ref, p_ref, psf_ref, t_ref, sems):
    copies = [
        pltpu.make_async_copy(src, dst, sems.at[k])
        for k, (src, dst) in enumerate(((psf_hbm, psf_ref.at[:DENSE]), (d_hbm, d_ref), (p_hbm, p_ref)))
    ]
    for copy in copies:
        copy.start()
    t_ref[DENSE:, :] = jnp.zeros((384 - DENSE, 128), jnp.float32)
    copies[0].wait()
    t_ref[:DENSE, :TAPS] = psf_ref[:DENSE, 0, :]
    turned = t_ref[...].T
    sent = (first_ref, second_ref)
    rest = turned[:TAPS, 256:]
    rest = jnp.where(lax.broadcasted_iota(jnp.int32, rest.shape, 1) < DENSE - 256, rest, 0.0)
    for ref in sent + (xfirst_ref, xsecond_ref):
        at = T * H
        ref[at : at + TAPS, :] = turned[:TAPS, :128]
        ref[at + TAPS : at + 2 * TAPS, :] = turned[:TAPS, 128:256]
        ref[at + 34 : at + 40, :] = rest[:6] + pltpu.roll(rest, FOLD, 1)[6:12]
        ref[at + 34 : at + 39, :] += pltpu.roll(rest, 2 * FOLD, 1)[12:17]
    copies[1].wait()
    copies[2].wait()
    v_ref[...] = d_ref[...] * p_ref[...]

    columns(v_ref, sent)
    rows(v_ref, (xfirst_ref, xsecond_ref))


def widen(v_ref, arrived, wide_ref):
    wide_ref[:, H : H + T, :] = v_ref[...]

    def place(onward, back):
        wide_ref[:, :H, :] = arrived[back][: T * H, :].reshape(T, H, Z)
        wide_ref[:, H + T :, :] = arrived[onward][: T * H, :].reshape(T, H, Z)

    by_parity("gy", place)


def pack_first(v_ref, own_ref, a_ref, b_ref, wide_ref, first_ref, second_ref):
    widen(v_ref, (a_ref, b_ref), wide_ref)

    def kernels(onward, back):
        for ref in (first_ref, second_ref):
            ref[T * H :, :] = jnp.where(last("gy"), own_ref[T * H :, :], (a_ref, b_ref)[onward][T * H :, :])

    by_parity("gy", kernels)
    corners(wide_ref, (first_ref, second_ref))


def pack_next(v_ref, a_ref, b_ref, wide_ref, first_ref, second_ref):
    widen(v_ref, (a_ref, b_ref), wide_ref)
    sent = (first_ref, second_ref)

    def place(onward, back):
        sent[onward][...] = wide_ref[H:]
        sent[back][...] = wide_ref[:H]

    by_parity("gx", place)


def halves(v):
    high = v.astype(jnp.bfloat16)
    low = (v - high.astype(jnp.float32)).astype(jnp.bfloat16)
    return jnp.concatenate([high, low], axis=1)


def stationary(v):
    both = halves(v)
    return jnp.concatenate([both, both], axis=0)


def expanded(rows):
    fold = rows[34:40]
    source = (
        rows[:TAPS],
        rows[TAPS : 2 * TAPS],
        jnp.concatenate([fold, pltpu.roll(fold, 128 - FOLD, 1), pltpu.roll(fold, 128 - 2 * FOLD, 1)[:5]], axis=0),
    )
    lane = lax.broadcasted_iota(jnp.int32, (TAPS, 128), 1)
    tiles = []
    for u in range(5):
        tile = jnp.zeros((TAPS, 128), jnp.float32)
        for a in range(4 * u, min(4 * u + 4, TAPS)):
            begin, to = TAPS * a, GROUP * (a % 4)
            for k in sorted({begin // 128, (begin + TAPS - 1) // 128}):
                low, high = max(begin, 128 * k), min(begin + TAPS, 128 * (k + 1))
                shift = (to - begin) % 128
                moved = pltpu.roll(source[k], shift, 1) if shift else source[k]
                tile = jnp.where((lane >= to + low - begin) & (lane < to + high - begin), moved, tile)
        tiles.append(tile)
    return jnp.concatenate(tiles, axis=1)


def shifted(table, rows_ref, k):
    for r in range(4):
        rolled = table if r == 0 else pltpu.roll(table, GROUP * r, 1)
        for u in range(5):
            rows_ref[(k * 4 + r) * 5 + u, :TAPS, :] = rolled[:, u * 128 : (u + 1) * 128]


def onward_x(stay, pair):
    return jnp.where(last("gx"), stay, jnp.where(even("gx"), pair[0][T * H :, :], pair[1][T * H :, :]))


def empty_tiles(wa_ref, wb_ref):
    zero = jnp.zeros((T, 128), jnp.bfloat16)
    for q, ref, at in ((0, wa_ref, 3), (1, wb_ref, 0), (2, wb_ref, 1), (3, wa_ref, 0)):
        for part in (0, ref.shape[0] // 2):
            for c in range(TAPS):
                for r in range(4):
                    ref[at + part, pl.ds(place_of(4 * q + r, c), T), :] = zero


def place_of(x, c):
    return (((x // 8) * TAPS + c) * 8 + x % 8) * T


def begin(own_ref, nexty_ref, xa_ref, xb_ref, tables_ref, wa_ref, wb_ref):
    own, nexty = own_ref[T * H :, :], nexty_ref[T * H :, :]
    across = onward_x(own, (xa_ref, xb_ref)) - own
    for k, rows in enumerate((own, 0.25 * across, nexty - own)):
        shifted(expanded(rows), tables_ref, k)
    for r in range(4):
        for u in range(5):
            at = r * 5 + u
            tables_ref[at] = tables_ref[at] + ((r + 0.5) / 4) * tables_ref[at + 20]
    empty_tiles(wa_ref, wb_ref)


def build(own_ref, nexty_ref, arrived, corner, tables_ref, wa_ref, wb_ref, rows_ref, even_ref, odd_ref, use):
    own, nexty = own_ref[T * H :, :], nexty_ref[T * H :, :]
    across = onward_x(own, arrived) - own
    shifted(expanded(0.25 * (onward_x(nexty, corner) - nexty - across)), rows_ref, 1)
    for r in range(4):
        for u in range(5):
            at = r * 5 + u
            rows_ref[at] = tables_ref[at + 40] + ((r + 0.5) / 4) * rows_ref[at + 20]
    along = lax.broadcasted_iota(jnp.int32, (H, Z), 0).astype(jnp.float32)
    steps = [(along + (0.5 + H * half)) / T for half in range(2)]

    def spread(c, q_ref):
        for r in range(4):
            for u in range(5):
                for m in range(2):
                    at = (m * 4 + r) * 5 + u
                    near = tables_ref[at, pl.ds(c, H, stride=0), :]
                    step = rows_ref[at, pl.ds(c, H, stride=0), :]
                    for half in range(2):
                        q_ref[m, r * 5 + u, half * H : (half + 1) * H, :] = pltpu.roll(
                            near + steps[half] * step, H * half, 1, stride=1, stride_axis=0
                        )

    def fill(c, q_ref):
        for r in range(4):
            for u in range(5):
                w, quarter = q_ref[0, r * 5 + u], q_ref[1, r * 5 + u]
                for q in range(4):
                    w = w if q == 0 else w + quarter
                    high = w.astype(jnp.bfloat16)
                    low = (w - high.astype(jnp.float32)).astype(jnp.bfloat16)
                    tile = q + u
                    rows = pl.ds(place_of(4 * q + r, c), T)
                    ref, at, width = (wa_ref, tile - 2, 4) if 2 <= tile < 6 else (wb_ref, tile % 2, 2)
                    ref[at, rows, :] = high
                    ref[at + width, rows, :] = low

    held_refs = (even_ref, odd_ref)
    spread(0, even_ref)
    spread(1, odd_ref)
    fill(0, even_ref)
    for c in range(TAPS):
        use(c)
        if c + 1 < TAPS:
            fill(c + 1, held_refs[(c + 1) % 2])
        if c + 2 < TAPS:
            spread(c + 2, held_refs[c % 2])


def joined(ref, rows):
    return jnp.concatenate([ref[t, rows, :] for t in range(ref.shape[0])], axis=1)


def product(w, v):
    both = jnp.dot(w, v, preferred_element_type=jnp.float32)
    return both[:, :Z] + both[:, Z:]


def inner_part(wide_ref, wa_ref, r_ref):
    v = stationary(wide_ref[...].reshape(T * GROUP, Z))
    for h in range(2):
        rows = slice(h * TAPS * 128, (h + 1) * TAPS * 128)
        r_ref[rows, :] = product(joined(wa_ref, rows), v)


def moved(part, c):
    if c == H:
        return part
    lane = lax.broadcasted_iota(jnp.int32, part.shape, 1)
    return jnp.where((lane >= H - c) & (lane < Z + H - c), pltpu.roll(part, (H - c) % Z, 1), 0.0)


def sides(arrived, corner, side_ref):
    def place(onward, back):
        for h, k in ((0, back), (1, onward)):
            ends = corner[k][: T * H, :].reshape(H, T, Z)
            side_ref[h, :, :H, :] = ends[:, :H]
            side_ref[h, :, H : H + T, :] = arrived[k][: T * H, :].reshape(H, T, Z)
            side_ref[h, :, H + T :, :] = ends[:, H:]

    by_parity("gx", place)


def outer_part(arrived, wb_ref, r_ref, out_ref, side_ref):
    def place(onward, back):
        side_ref[0] = arrived[back][...]
        side_ref[1] = arrived[onward][...]

    by_parity("gx", place)
    for h in range(2):
        v = stationary(side_ref[h].reshape(H * GROUP, Z))
        total = None
        for c in range(TAPS):
            at = slice((h * TAPS + c) * 128, (h * TAPS + c + 1) * 128)
            part = moved(r_ref[at, :] + product(joined(wb_ref, at), v), c)
            total = part if total is None else total + part
        out_ref[h * 8 : (h + 1) * 8] = total.reshape(8, T, Z)


def step_one(d_ref, p_ref, wide_ref, own_ref, nexty_ref, xa_ref, xb_ref, ca_ref, cb_ref, tables_ref, wa_in, wb_in,
             wa_ref, wb_ref, model_ref, first_ref, second_ref, rows_ref,
             even_ref, odd_ref, all_ref, k_ref, side_ref):
    arrived, corner = (xa_ref, xb_ref), (ca_ref, cb_ref)
    sides(arrived, corner, side_ref)
    inner = stationary(wide_ref[...].reshape(T * GROUP, Z))
    for h in range(2):
        all_ref[h, : 4 * 256, :] = inner
        all_ref[h, 4 * 256 :, :] = stationary(side_ref[h].reshape(H * GROUP, Z))

    def use(c):
        for h in range(2):
            at = slice((h * TAPS + c) * 128, (h * TAPS + c + 1) * 128)
            w = jnp.concatenate([joined(wa_ref, at), joined(wb_ref, at)], axis=1)
            part = moved(product(w, all_ref[h]), c)
            k_ref[h] = part if c == 0 else k_ref[h] + part

    build(own_ref, nexty_ref, arrived, corner, tables_ref, wa_ref, wb_ref, rows_ref, even_ref, odd_ref, use)
    v = wide_ref[:, H : H + T, :]
    residual = d_ref[...] - (v + k_ref[...].reshape(T, T, Z))
    model_ref[...] = v + relaxation * p_ref[...] * residual
    columns(model_ref, (first_ref, second_ref))


def step_two(d_ref, p_ref, v_ref, a_ref, b_ref, wb_ref, r_ref, model_ref, residual_ref, k_ref, side_ref):
    outer_part((a_ref, b_ref), wb_ref, r_ref, k_ref, side_ref)
    v = v_ref[...]
    residual = d_ref[...] - (v + k_ref[...])
    residual_ref[...] = residual
    model_ref[...] = v + relaxation * p_ref[...] * residual


def local(data, precond, psf):
    wide_shape = held(T, GROUP, Z)
    block = pltpu.VMEM((T, T, Z), jnp.float32)
    edges = pltpu.VMEM((2, H, GROUP, Z), jnp.float32)
    row, tile = held(T * H + PACKED, Z), held(T, T, Z)
    psf = psf.reshape(DENSE, 1, TAPS)
    v, first, second, xfirst, xsecond, data, precond = call(
        prepare,
        (tile, row, row, row, row, tile, tile),
        4,
        [
            pltpu.VMEM((DENSE + 7, 1, TAPS), jnp.float32),
            pltpu.VMEM((384, 128), jnp.float32),
            pltpu.SemaphoreType.DMA((3,)),
        ],
        pl.BlockSpec(memory_space=pltpu.HBM),
    )(*(pltpu.with_memory_space_constraint(x, pltpu.HBM) for x in (data, precond, psf)))
    a, b = swapped("gy", first, second)
    xa, xb = swapped("gx", xfirst, xsecond)
    wide, cfirst, csecond = call(pack_first, (wide_shape, row, row), 3)(*map(keep, (v, first, a, b)))
    ca, cb = swapped("gx", cfirst, csecond)
    wa, wb = held(8, ROWS, 128, dtype=jnp.bfloat16), held(4, ROWS, 128, dtype=jnp.bfloat16)
    tables, wa_zero, wb_zero = call(begin, (held(60, 24, 128), wa, wb), 2)(*map(keep, (first, cfirst, xa, xb)))
    row = held(T * H, Z)
    turned = pltpu.VMEM((2, 20, T, 128), jnp.float32)
    wa, wb, v, first, second = call(
        step_one,
        (wa, wb, tile, row, row),
        14,
        [
            pltpu.VMEM((40, 24, 128), jnp.float32),
            turned,
            turned,
            pltpu.VMEM((2, 6 * 256, 2 * Z), jnp.bfloat16),
            pltpu.VMEM((2, 128, Z), jnp.float32),
            edges,
        ],
        alias={10: 0, 11: 1},
    )(*map(keep, (data, precond, wide, first, cfirst, xa, xb, ca, cb, tables, wa_zero, wb_zero)))
    a, b = swapped("gy", first, second)
    edge = held(H, GROUP, Z)
    wide, first, second = call(pack_next, (wide_shape, edge, edge), 3)(*map(keep, (v, a, b)))
    a, b = swapped("gx", first, second)
    part = call(inner_part, held(ROWS, Z), 8)(*map(keep, (wide, wa)))
    return call(step_two, (f32(T, T, Z), f32(T, T, Z)), 6, [block, edges])(
        *map(keep, (data, precond, v, a, b, wb, part))
    )


def solution(mesh):
    placed = (P("gx", "gy", None), P("gx", "gy", None), P("gx", "gy", None, None, None))
    return jax.shard_map(
        local,
        mesh=mesh,
        in_specs=placed,
        out_specs=(P("gx", "gy", None), P("gx", "gy", None)),
        check_vma=False,
    )
```

```python
import jax
import jax.numpy as jnp
from jax import lax
from jax.experimental import pallas as pl
from jax.experimental.pallas import tpu as pltpu
from jax.sharding import PartitionSpec as P


relaxation = 0.7

H = 8
TAPS = 17
T = 16
Z = 128
GROUP = 32
DENSE = TAPS * TAPS
ROWS = 2 * TAPS * 8 * T
PACKED = 40
FOLD = 40
VMEM = pl.BlockSpec(memory_space=pltpu.VMEM)
MIB = 1 << 20


def held(*shape, dtype=jnp.float32):
    return pltpu.VMEM(shape, dtype)


def keep(x):
    return pltpu.with_memory_space_constraint(x, pltpu.VMEM)


def call(kernel, outs, mib, scratch=(), space=VMEM, alias={}):
    def run(*operands):
        return pl.pallas_call(
            kernel,
            out_shape=outs,
            in_specs=[space] * len(operands),
            out_specs=jax.tree.map(lambda _: VMEM, outs),
            scratch_shapes=list(scratch),
            input_output_aliases=alias,
            compiler_params=pltpu.CompilerParams(vmem_limit_bytes=int(mib * MIB)),
        )(*operands)

    return run


def even(axis):
    return lax.axis_index(axis) % 2 == 0


def last(axis):
    return lax.axis_index(axis) == lax.axis_size(axis) - 1


def swapped(axis, first, second):
    size = lax.axis_size(axis)
    received = []
    for start, sent in ((0, first), (1, second)):
        pairs = []
        for i in range(start, size - 1, 2):
            pairs += [(i, i + 1), (i + 1, i)]
        received.append(lax.ppermute(sent, axis, pairs))
    return received


def by_parity(axis, action):
    pl.when(even(axis))(lambda: action(0, 1))
    pl.when(jnp.logical_not(even(axis)))(lambda: action(1, 0))


def f32(*shape):
    return jax.ShapeDtypeStruct(shape, jnp.float32)


def columns(v_ref, sent):
    def place(onward, back):
        sent[onward][: T * H, :] = v_ref[:, H:, :].reshape(T * H, Z)
        sent[back][: T * H, :] = v_ref[:, :H, :].reshape(T * H, Z)

    by_parity("gy", place)


def rows(v_ref, sent):
    def place(onward, back):
        sent[onward][: T * H, :] = v_ref[H:].reshape(T * H, Z)
        sent[back][: T * H, :] = v_ref[:H].reshape(T * H, Z)

    by_parity("gx", place)


def corners(wide_ref, sent):
    def place(onward, back):
        for ref, half in ((sent[onward], wide_ref.at[H:]), (sent[back], wide_ref.at[:H])):
            ref[: T * H, :] = jnp.concatenate([half[:, :H, :], half[:, H + T :, :]], axis=1).reshape(T * H, Z)

    by_parity("gx", place)


def prepare(d_hbm, p_hbm, psf_hbm, v_ref, first_ref, second_ref, xfirst_ref, xsecond_ref, d_ref, p_ref, psf_ref, t_ref, sems):
    copies = [
        pltpu.make_async_copy(src, dst, sems.at[k])
        for k, (src, dst) in enumerate(((psf_hbm, psf_ref.at[:DENSE]), (d_hbm, d_ref), (p_hbm, p_ref)))
    ]
    for copy in copies:
        copy.start()
    t_ref[DENSE:, :] = jnp.zeros((384 - DENSE, 128), jnp.float32)
    copies[0].wait()
    t_ref[:DENSE, :TAPS] = psf_ref[:DENSE, 0, :]
    turned = t_ref[...].T
    sent = (first_ref, second_ref)
    rest = turned[:TAPS, 256:]
    rest = jnp.where(lax.broadcasted_iota(jnp.int32, rest.shape, 1) < DENSE - 256, rest, 0.0)
    for ref in sent + (xfirst_ref, xsecond_ref):
        at = T * H
        ref[at : at + TAPS, :] = turned[:TAPS, :128]
        ref[at + TAPS : at + 2 * TAPS, :] = turned[:TAPS, 128:256]
        ref[at + 34 : at + 40, :] = rest[:6] + pltpu.roll(rest, FOLD, 1)[6:12]
        ref[at + 34 : at + 39, :] += pltpu.roll(rest, 2 * FOLD, 1)[12:17]
    copies[1].wait()
    copies[2].wait()
    v_ref[...] = d_ref[...] * p_ref[...]

    columns(v_ref, sent)
    rows(v_ref, (xfirst_ref, xsecond_ref))


def widen(v_ref, arrived, wide_ref):
    wide_ref[:, H : H + T, :] = v_ref[...]

    def place(onward, back):
        wide_ref[:, :H, :] = arrived[back][: T * H, :].reshape(T, H, Z)
        wide_ref[:, H + T :, :] = arrived[onward][: T * H, :].reshape(T, H, Z)

    by_parity("gy", place)


def pack_first(v_ref, own_ref, a_ref, b_ref, wide_ref, first_ref, second_ref):
    widen(v_ref, (a_ref, b_ref), wide_ref)

    def kernels(onward, back):
        for ref in (first_ref, second_ref):
            ref[T * H :, :] = jnp.where(last("gy"), own_ref[T * H :, :], (a_ref, b_ref)[onward][T * H :, :])

    by_parity("gy", kernels)
    corners(wide_ref, (first_ref, second_ref))


def pack_next(v_ref, a_ref, b_ref, wide_ref, first_ref, second_ref):
    widen(v_ref, (a_ref, b_ref), wide_ref)
    sent = (first_ref, second_ref)

    def place(onward, back):
        sent[onward][...] = wide_ref[H:]
        sent[back][...] = wide_ref[:H]

    by_parity("gx", place)


def halves(v):
    high = v.astype(jnp.bfloat16)
    low = (v - high.astype(jnp.float32)).astype(jnp.bfloat16)
    return jnp.concatenate([high, low], axis=1)


def stationary(v):
    both = halves(v)
    return jnp.concatenate([both, both], axis=0)


def expanded(rows):
    fold = rows[34:40]
    source = (
        rows[:TAPS],
        rows[TAPS : 2 * TAPS],
        jnp.concatenate([fold, pltpu.roll(fold, 128 - FOLD, 1), pltpu.roll(fold, 128 - 2 * FOLD, 1)[:5]], axis=0),
    )
    lane = lax.broadcasted_iota(jnp.int32, (TAPS, 128), 1)
    tiles = []
    for u in range(5):
        tile = jnp.zeros((TAPS, 128), jnp.float32)
        for a in range(4 * u, min(4 * u + 4, TAPS)):
            begin, to = TAPS * a, GROUP * (a % 4)
            for k in sorted({begin // 128, (begin + TAPS - 1) // 128}):
                low, high = max(begin, 128 * k), min(begin + TAPS, 128 * (k + 1))
                shift = (to - begin) % 128
                moved = pltpu.roll(source[k], shift, 1) if shift else source[k]
                tile = jnp.where((lane >= to + low - begin) & (lane < to + high - begin), moved, tile)
        tiles.append(tile)
    return jnp.concatenate(tiles, axis=1)


def shifted(table, rows_ref, k):
    for r in range(4):
        rolled = table if r == 0 else pltpu.roll(table, GROUP * r, 1)
        for u in range(5):
            rows_ref[(k * 4 + r) * 5 + u, :TAPS, :] = rolled[:, u * 128 : (u + 1) * 128]


def onward_x(stay, pair):
    return jnp.where(last("gx"), stay, jnp.where(even("gx"), pair[0][T * H :, :], pair[1][T * H :, :]))


def empty_tiles(wa_ref, wb_ref):
    zero = jnp.zeros((T, 128), jnp.bfloat16)
    for q, ref, at in ((0, wa_ref, 3), (1, wb_ref, 0), (2, wb_ref, 1), (3, wa_ref, 0)):
        for part in (0, ref.shape[0] // 2):
            for c in range(TAPS):
                for r in range(4):
                    ref[at + part, pl.ds(place_of(4 * q + r, c), T), :] = zero


def place_of(x, c):
    return (((x // 8) * TAPS + c) * 8 + x % 8) * T


def begin(own_ref, nexty_ref, xa_ref, xb_ref, tables_ref, wa_ref, wb_ref):
    own, nexty = own_ref[T * H :, :], nexty_ref[T * H :, :]
    across = onward_x(own, (xa_ref, xb_ref)) - own
    for k, rows in enumerate((own, 0.25 * across, nexty - own)):
        shifted(expanded(rows), tables_ref, k)
    for r in range(4):
        for u in range(5):
            at = r * 5 + u
            tables_ref[at] = tables_ref[at] + ((r + 0.5) / 4) * tables_ref[at + 20]
    empty_tiles(wa_ref, wb_ref)


def build(own_ref, nexty_ref, arrived, corner, tables_ref, wa_ref, wb_ref, rows_ref, even_ref, odd_ref, use):
    own, nexty = own_ref[T * H :, :], nexty_ref[T * H :, :]
    across = onward_x(own, arrived) - own
    shifted(expanded(0.25 * (onward_x(nexty, corner) - nexty - across)), rows_ref, 1)
    for r in range(4):
        for u in range(5):
            at = r * 5 + u
            rows_ref[at] = tables_ref[at + 40] + ((r + 0.5) / 4) * rows_ref[at + 20]
    along = lax.broadcasted_iota(jnp.int32, (H, Z), 0).astype(jnp.float32)
    steps = [(along + (0.5 + H * half)) / T for half in range(2)]

    def spread(c, q_ref):
        for r in range(4):
            for u in range(5):
                for m in range(2):
                    at = (m * 4 + r) * 5 + u
                    near = tables_ref[at, pl.ds(c, H, stride=0), :]
                    step = rows_ref[at, pl.ds(c, H, stride=0), :]
                    for half in range(2):
                        q_ref[m, r * 5 + u, half * H : (half + 1) * H, :] = pltpu.roll(
                            near + steps[half] * step, H * half, 1, stride=1, stride_axis=0
                        )

    def fill(c, q_ref):
        for r in range(4):
            for u in range(5):
                w, quarter = q_ref[0, r * 5 + u], q_ref[1, r * 5 + u]
                for q in range(4):
                    w = w if q == 0 else w + quarter
                    high = w.astype(jnp.bfloat16)
                    low = (w - high.astype(jnp.float32)).astype(jnp.bfloat16)
                    tile = q + u
                    rows = pl.ds(place_of(4 * q + r, c), T)
                    ref, at, width = (wa_ref, tile - 2, 4) if 2 <= tile < 6 else (wb_ref, tile % 2, 2)
                    ref[at, rows, :] = high
                    ref[at + width, rows, :] = low

    held_refs = (even_ref, odd_ref)
    spread(0, even_ref)
    spread(1, odd_ref)
    fill(0, even_ref)
    for c in range(TAPS):
        use(c)
        if c + 1 < TAPS:
            fill(c + 1, held_refs[(c + 1) % 2])
        if c + 2 < TAPS:
            spread(c + 2, held_refs[c % 2])


def joined(ref, rows):
    return jnp.concatenate([ref[t, rows, :] for t in range(ref.shape[0])], axis=1)


def product(w, v):
    both = jnp.dot(w, v, preferred_element_type=jnp.float32)
    return both[:, :Z] + both[:, Z:]


def inner_part(wide_ref, wa_ref, r_ref):
    v = stationary(wide_ref[...].reshape(T * GROUP, Z))
    for h in range(2):
        rows = slice(h * TAPS * 128, (h + 1) * TAPS * 128)
        r_ref[rows, :] = product(joined(wa_ref, rows), v)


def moved(part, c):
    if c == H:
        return part
    lane = lax.broadcasted_iota(jnp.int32, part.shape, 1)
    return jnp.where((lane >= H - c) & (lane < Z + H - c), pltpu.roll(part, (H - c) % Z, 1), 0.0)


def sides(arrived, corner, side_ref):
    def place(onward, back):
        for h, k in ((0, back), (1, onward)):
            ends = corner[k][: T * H, :].reshape(H, T, Z)
            side_ref[h, :, :H, :] = ends[:, :H]
            side_ref[h, :, H : H + T, :] = arrived[k][: T * H, :].reshape(H, T, Z)
            side_ref[h, :, H + T :, :] = ends[:, H:]

    by_parity("gx", place)


def outer_part(arrived, wb_ref, r_ref, out_ref, side_ref):
    def place(onward, back):
        side_ref[0] = arrived[back][...]
        side_ref[1] = arrived[onward][...]

    by_parity("gx", place)
    for h in range(2):
        v = stationary(side_ref[h].reshape(H * GROUP, Z))
        total = None
        for c in range(TAPS):
            at = slice((h * TAPS + c) * 128, (h * TAPS + c + 1) * 128)
            part = moved(r_ref[at, :] + product(joined(wb_ref, at), v), c)
            total = part if total is None else total + part
        out_ref[h * 8 : (h + 1) * 8] = total.reshape(8, T, Z)


def step_one(d_ref, p_ref, wide_ref, own_ref, nexty_ref, xa_ref, xb_ref, ca_ref, cb_ref, tables_ref, wa_in, wb_in,
             wa_ref, wb_ref, model_ref, first_ref, second_ref, rows_ref,
             even_ref, odd_ref, inner_ref, outer_ref, k_ref, side_ref):
    arrived, corner = (xa_ref, xb_ref), (ca_ref, cb_ref)
    sides(arrived, corner, side_ref)
    inner_ref[...] = halves(wide_ref[...].reshape(T * GROUP, Z))
    for h in range(2):
        outer_ref[h] = halves(side_ref[h].reshape(H * GROUP, Z))

    def use(c):
        for h in range(2):
            at = slice((h * TAPS + c) * 128, (h * TAPS + c + 1) * 128)
            w = jnp.concatenate([joined(wa_ref, at), joined(wb_ref, at)], axis=1)
            part = moved(product(w, jnp.concatenate([inner_ref[...]] * 2 + [outer_ref[h]] * 2, axis=0)), c)
            k_ref[h] = part if c == 0 else k_ref[h] + part

    build(own_ref, nexty_ref, arrived, corner, tables_ref, wa_ref, wb_ref, rows_ref, even_ref, odd_ref, use)
    v = wide_ref[:, H : H + T, :]
    residual = d_ref[...] - (v + k_ref[...].reshape(T, T, Z))
    model_ref[...] = v + relaxation * p_ref[...] * residual
    columns(model_ref, (first_ref, second_ref))


def step_two(d_ref, p_ref, v_ref, a_ref, b_ref, wb_ref, r_ref, model_ref, residual_ref, k_ref, side_ref):
    outer_part((a_ref, b_ref), wb_ref, r_ref, k_ref, side_ref)
    v = v_ref[...]
    residual = d_ref[...] - (v + k_ref[...])
    residual_ref[...] = residual
    model_ref[...] = v + relaxation * p_ref[...] * residual


def local(data, precond, psf):
    wide_shape = held(T, GROUP, Z)
    block = pltpu.VMEM((T, T, Z), jnp.float32)
    edges = pltpu.VMEM((2, H, GROUP, Z), jnp.float32)
    row, tile = held(T * H + PACKED, Z), held(T, T, Z)
    psf = psf.reshape(DENSE, 1, TAPS)
    v, first, second, xfirst, xsecond, data, precond = call(
        prepare,
        (tile, row, row, row, row, tile, tile),
        4,
        [
            pltpu.VMEM((DENSE + 7, 1, TAPS), jnp.float32),
            pltpu.VMEM((384, 128), jnp.float32),
            pltpu.SemaphoreType.DMA((3,)),
        ],
        pl.BlockSpec(memory_space=pltpu.HBM),
    )(*(pltpu.with_memory_space_constraint(x, pltpu.HBM) for x in (data, precond, psf)))
    a, b = swapped("gy", first, second)
    xa, xb = swapped("gx", xfirst, xsecond)
    wide, cfirst, csecond = call(pack_first, (wide_shape, row, row), 3)(*map(keep, (v, first, a, b)))
    ca, cb = swapped("gx", cfirst, csecond)
    wa, wb = held(8, ROWS, 128, dtype=jnp.bfloat16), held(4, ROWS, 128, dtype=jnp.bfloat16)
    tables, wa_zero, wb_zero = call(begin, (held(60, 24, 128), wa, wb), 2)(*map(keep, (first, cfirst, xa, xb)))
    row = held(T * H, Z)
    turned = pltpu.VMEM((2, 20, T, 128), jnp.float32)
    wa, wb, v, first, second = call(
        step_one,
        (wa, wb, tile, row, row),
        14,
        [
            pltpu.VMEM((40, 24, 128), jnp.float32),
            turned,
            turned,
            pltpu.VMEM((T * GROUP, 2 * Z), jnp.bfloat16),
            pltpu.VMEM((2, H * GROUP, 2 * Z), jnp.bfloat16),
            pltpu.VMEM((2, 128, Z), jnp.float32),
            edges,
        ],
        alias={10: 0, 11: 1},
    )(*map(keep, (data, precond, wide, first, cfirst, xa, xb, ca, cb, tables, wa_zero, wb_zero)))
    a, b = swapped("gy", first, second)
    edge = held(H, GROUP, Z)
    wide, first, second = call(pack_next, (wide_shape, edge, edge), 3)(*map(keep, (v, a, b)))
    a, b = swapped("gx", first, second)
    part = call(inner_part, held(ROWS, Z), 8)(*map(keep, (wide, wa)))
    return call(step_two, (f32(T, T, Z), f32(T, T, Z)), 6, [block, edges])(
        *map(keep, (data, precond, v, a, b, wb, part))
    )


def solution(mesh):
    placed = (P("gx", "gy", None), P("gx", "gy", None), P("gx", "gy", None, None, None))
    return jax.shard_map(
        local,
        mesh=mesh,
        in_specs=placed,
        out_specs=(P("gx", "gy", None), P("gx", "gy", None)),
        check_vma=False,
    )
```
